32 devices in a mesh: row: 4 (over x, core), col: 8 (over z, y).
Axes of the slice: x: 2, y: 2, z: 4, core: 2. Of those that a mesh axis runs over, the one named last changes fastest.
Arguments:
- tensor: float32 [1024, 32, 1024], P(None, 'row', 'col'), may hold values from -60 to 60, as said below
- factor_two: float32 [32, 32], P('row'), may hold values from -1 to 1
- factor_three: float32 [32, 32], P('col'), may hold values from -1 to 1
- factor_four: float32 [32, 16], replicated, may hold values from -1 to 1
- factor_init: float32 [1024, 64], replicated, may hold values from -6 to 6
Outputs:
- factor_new: float32 [1024, 64], replicated
- core: float32 [64, 32, 32, 16], P(None, 'row', 'col')
The draws below stay inside these ranges and needn't reach their ends.
Inputs may be any that keep to these rules, and one draw needn't show every extreme that they name: `tensor`: scales vary from slab to slab.
All inputs are finite; a program needn't handle non-finite values.
Results may differ from the reference program's by a relative error of at most 0.00013.
Values sent between devices are 32-bit elements; how exact they have to be, the bound alone decides.
A program may use at most 128 MiB of HBM per device.

```python
import jax
import jax.numpy as jnp
from jax import lax

I1 = 1024
I4 = 32
R1 = 64
R2 = 32
R3 = 32
R4 = 16
ITERS = 1
I2 = 32
I3 = 32


def draw_tensor(key, part):
    first, second = jax.random.split(jax.random.fold_in(key, 11), 2)
    shape = (I1, I2, I3 * I4)
    base = jnp.clip(jax.random.normal(first, shape, jnp.float32), -6.0, 6.0)
    ramp_two = jnp.arange(I2, dtype=jnp.float32) / max(I2 - 1, 1)
    ramp_three = jnp.arange(I3, dtype=jnp.float32) / max(I3 - 1, 1)
    logs = jax.random.uniform(second, (I2, I3), jnp.float32) + 0.5 * ramp_two[:, None] + 0.5 * ramp_three[None, :] - 1.0
    scales = jnp.repeat(10.0 ** logs, I4, axis=1)
    values = base * scales[None, :, :]
    return jnp.clip(values, -60.0, 60.0)


def levels(key, dims, cuts, smallest, high):
    loudness = 1.0
    for dim, blocks in cuts:
        draws = jax.random.uniform(jax.random.fold_in(jax.random.fold_in(key, 6), dim), (blocks,), jnp.float32, smallest / len(cuts), high / len(cuts))
        loudness = loudness * jnp.repeat(jnp.exp(draws), dims[dim] // blocks).reshape((-1,) + (1,) * (len(dims) - 1 - dim))
    return loudness


def bell_draw(rng, extent, spread, limit, shards=(), kind=jnp.bfloat16):
    level = levels(rng, extent, shards, -0.22, 0.18) if shards else 1.0
    array = jax.random.normal(rng, extent, jnp.float32) * spread * level
    return jnp.minimum(jnp.maximum(array, -limit), limit).astype(kind)


def setup_inputs(seed: int = 0) -> dict:
    key_list = jax.random.split(jax.random.key(seed), 6)
    tensor = draw_tensor(jax.random.fold_in(key_list[5], 71), 0)
    factor_two = bell_draw(key_list[1], (I2, R2), I2 ** -0.5, 1.0, ((0, 4),), jnp.float32)
    factor_three = bell_draw(key_list[2], (I3, R3), I3 ** -0.5, 1.0, ((0, 8),), jnp.float32)
    factor_four = bell_draw(key_list[3], (I4, R4), I4 ** -0.5, 1.0, (), jnp.float32)
    factor_init = bell_draw(key_list[4], (I1, R1), 1.0, 6.0, (), jnp.float32)
    return dict(tensor=tensor, factor_two=factor_two, factor_three=factor_three, factor_four=factor_four, factor_init=factor_init)


def reference(tensor, factor_two, factor_three, factor_four, factor_init):
    highest = lax.Precision.HIGHEST
    data = tensor.reshape(I1, I2, I3, I4)
    fourth = jnp.einsum('abcd,de->abce', data, factor_four, precision=highest)
    third = jnp.einsum('abce,cf->abfe', fourth, factor_three, precision=highest)
    projected = jnp.einsum('abfe,bg->agfe', third, factor_two, precision=highest)
    unfolded = projected.reshape(I1, R2 * R3 * R4)
    gram = jnp.dot(unfolded.astype(jnp.float32), unfolded.T.astype(jnp.float32), precision=highest, preferred_element_type=jnp.float32)
    basis = factor_init
    for step in range(ITERS):
        image = jnp.dot(gram.astype(jnp.float32), basis.astype(jnp.float32), precision=highest, preferred_element_type=jnp.float32)
        square = jnp.dot(image.T.astype(jnp.float32), image.astype(jnp.float32), precision=highest, preferred_element_type=jnp.float32)
        lower = jnp.linalg.cholesky(square)
        basis = jax.scipy.linalg.solve_triangular(lower, image.T, lower=True).T
    core = jnp.dot(basis.T.astype(jnp.float32), unfolded.astype(jnp.float32), precision=highest, preferred_element_type=jnp.float32)
    return (basis, core.reshape(R1, R2, R3, R4))
```

```python
import jax
import jax.numpy as jnp
from jax import lax
from jax.experimental import pallas as pl
from jax.experimental.pallas import tpu as pltpu
from jax.sharding import PartitionSpec as P

HIGHEST = lax.Precision.HIGHEST


def dot(a, b, dims):
    return lax.dot_general(a, b, (dims, ((), ())), precision=HIGHEST, preferred_element_type=jnp.float32)


def inverse_factor(square):
    size = square.shape[0]
    rows = lax.broadcasted_iota(jnp.int32, (size, size), 0)
    cols = lax.broadcasted_iota(jnp.int32, (size, size), 1)
    index = lax.broadcasted_iota(jnp.int32, (size, 1), 0)
    left = square
    right = jnp.where(rows == cols, 1.0, 0.0).astype(jnp.float32)
    for k in range(size):
        scale = lax.rsqrt(left[k:k + 1, k:k + 1])
        column = left[:, k:k + 1] * scale
        pivot_left = left[k:k + 1, :] * scale
        pivot_right = right[k:k + 1, :] * scale
        factor = jnp.where(index > k, column, 0.0)
        left = left - factor * pivot_left
        right = jnp.where(index == k, pivot_right, right - factor * pivot_right)
    return right


def finish_kernel(image_ref, basis_ref, inverse_ref):
    image = image_ref[...]
    inverse = inverse_factor(dot(image, image, ((0,), (0,))))
    inverse_ref[...] = inverse
    basis_ref[...] = dot(image, inverse, ((1,), (1,)))


def finish(image):
    rank = image.shape[1]
    return pl.pallas_call(
        finish_kernel,
        out_shape=(
            jax.ShapeDtypeStruct(image.shape, jnp.float32),
            jax.ShapeDtypeStruct((rank, rank), jnp.float32),
        ),
    )(image)


def shards(tensor, factor_two, factor_three, factor_four, factor_init):
    axes = ("row", "col")
    first_len, local_two, width = tensor.shape
    fourth_len, rank_four = factor_four.shape
    local_three = width // fourth_len
    rank_one = factor_init.shape[1]
    rows, cols = lax.axis_size("row"), lax.axis_size("col")
    devices = rows * cols
    local_pairs = local_two * local_three
    features = rank_four * rank_one
    part = features // devices
    data = tensor.reshape(first_len, local_pairs, fourth_len)
    whole_two = lax.all_gather(factor_two, "row", axis=0, tiled=True)
    whole_three = lax.all_gather(factor_three, "col", axis=0, tiled=True)
    whole_two_len, rank_two = whole_two.shape
    whole_three_len, rank_three = whole_three.shape

    def pull(vectors):
        mixed = jnp.einsum("apd,ar->prd", data, vectors, precision=HIGHEST)
        return jnp.einsum("prd,de->per", mixed, factor_four, precision=HIGHEST).reshape(local_pairs, features)

    def spread(block):
        got = lax.all_to_all(block.reshape(local_pairs, devices, part).transpose(1, 0, 2), axes, 0, 0, tiled=True)
        got = got.reshape(rows, cols, local_two, local_three, part)
        return got.transpose(0, 2, 1, 3, 4).reshape(rows * local_two, cols * local_three, part)

    def gather(block):
        two, three, _ = block.shape
        put = block.reshape(rows, two // rows, cols, three // cols, part).transpose(0, 2, 1, 3, 4)
        put = put.reshape(devices, (two // rows) * (three // cols), part)
        got = lax.all_to_all(put, axes, 0, 0, tiled=True)
        return got.transpose(1, 0, 2).reshape(got.shape[1], features)

    block = spread(pull(factor_init))
    block = jnp.einsum("bcq,bg->gcq", block, whole_two, precision=HIGHEST)
    block = jnp.einsum("gcq,cf->gfq", block, whole_three, precision=HIGHEST)
    block = jnp.einsum("gfq,cf->gcq", block, whole_three, precision=HIGHEST)
    block = jnp.einsum("gcq,bg->bcq", block, whole_two, precision=HIGHEST)
    block = gather(block).reshape(local_pairs, rank_four, rank_one)
    block = jnp.einsum("per,de->pdr", block, factor_four, precision=HIGHEST)
    image = lax.psum(dot(tensor.reshape(first_len, -1), block.reshape(-1, rank_one), ((1,), (0,))), axes)
    basis, inverse = finish(image)
    block = spread(pull(image))
    block = jnp.einsum("bcq,bg->gcq", block, whole_two, precision=HIGHEST)
    block = jnp.einsum("gcq,cf->gfq", block, whole_three, precision=HIGHEST)
    block = gather(block).reshape(-1, rank_four, rank_one)
    core = jnp.einsum("per,sr->spe", block, inverse, precision=HIGHEST)
    return (basis, core.reshape(rank_one, rank_two // rows, rank_three // cols, rank_four))


def solution(mesh):
    in_specs = (P(None, "row", "col"), P("row", None), P("col", None), P(), P())
    out_specs = (P(), P(None, "row", "col", None))
    return jax.shard_map(shards, mesh=mesh, in_specs=in_specs, out_specs=out_specs, check_vma=False)
```

```python
import functools

import jax
import jax.numpy as jnp
from jax import lax
from jax.experimental import pallas as pl
from jax.experimental.pallas import tpu as pltpu
from jax.sharding import PartitionSpec as P

HIGHEST = lax.Precision.HIGHEST
LANES = 128


def dot(a, b, dims):
    return lax.dot_general(a, b, (dims, ((), ())), precision=HIGHEST, preferred_element_type=jnp.float32)


def inverse_factor(square):
    size = square.shape[0]
    rows = lax.broadcasted_iota(jnp.int32, (size, size), 0)
    cols = lax.broadcasted_iota(jnp.int32, (size, size), 1)
    index = lax.broadcasted_iota(jnp.int32, (size, 1), 0)
    left = square
    right = jnp.where(rows == cols, 1.0, 0.0).astype(jnp.float32)
    for k in range(size):
        scale = lax.rsqrt(left[k:k + 1, k:k + 1])
        column = left[:, k:k + 1] * scale
        pivot_left = left[k:k + 1, :] * scale
        pivot_right = right[k:k + 1, :] * scale
        factor = jnp.where(index > k, column, 0.0)
        left = left - factor * pivot_left
        right = jnp.where(index == k, pivot_right, right - factor * pivot_right)
    return right


def finish_kernel(image_ref, basis_ref, inverse_ref):
    image = image_ref[...]
    inverse = inverse_factor(dot(image, image, ((0,), (0,))))
    inverse_ref[...] = inverse
    basis_ref[...] = dot(image, inverse, ((1,), (1,)))


def finish(image):
    rank = image.shape[1]
    return pl.pallas_call(
        finish_kernel,
        out_shape=(
            jax.ShapeDtypeStruct(image.shape, jnp.float32),
            jax.ShapeDtypeStruct((rank, rank), jnp.float32),
        ),
    )(image)


def place():
    return lax.axis_index("row") * lax.axis_size("col") + lax.axis_index("col")


def greet(devices):
    cols = lax.axis_size("col")
    me = place()
    barrier = pltpu.get_barrier_semaphore()

    def hello(k, carry):
        peer = lax.rem(me + k, devices)
        pl.semaphore_signal(barrier, inc=1, device_id=(peer // cols, lax.rem(peer, cols)), device_id_type=pl.DeviceIdType.MESH)
        return carry

    lax.fori_loop(1, devices, hello, 0)
    pl.semaphore_wait(barrier, devices - 1)


def send_all(devices, source, target, send_sem, recv_sem):
    cols = lax.axis_size("col")
    me = place()

    def send(k, carry):
        peer = lax.rem(me + k, devices)
        pltpu.make_async_remote_copy(
            src_ref=source(peer),
            dst_ref=target.at[me],
            send_sem=send_sem,
            recv_sem=recv_sem,
            device_id=(peer // cols, lax.rem(peer, cols)),
            device_id_type=pl.DeviceIdType.MESH,
        ).start()
        return carry

    lax.fori_loop(1, devices, send, 0)
    whole = target.at[pl.ds(0, devices - 1)]
    pltpu.make_async_copy(whole, whole, send_sem).wait()
    pltpu.make_async_copy(whole, whole, recv_sem).wait()


def swap_kernel(devices, put_ref, out_ref, held, send_sem, recv_sem):
    me = place()
    greet(devices)
    send_all(devices, lambda peer: put_ref.at[peer], held, send_sem, recv_sem)
    held[me] = put_ref[me]
    out_ref[...] = held[...]


def total_kernel(devices, put_ref, out_ref, held, mine, spread, sems):
    me = place()
    greet(devices)
    send_all(devices, lambda peer: put_ref.at[peer], held, sems.at[0], sems.at[1])
    held[me] = put_ref[me]
    mine[...] = jnp.sum(held[...], axis=0)
    send_all(devices, lambda peer: mine, spread, sems.at[2], sems.at[3])
    spread[me] = mine[...]
    out_ref[...] = spread[...]


def swap(values, ident):
    devices = values.shape[0]
    return pl.pallas_call(
        functools.partial(swap_kernel, devices),
        out_shape=jax.ShapeDtypeStruct(values.shape, jnp.float32),
        in_specs=[pl.BlockSpec(memory_space=pltpu.VMEM)],
        out_specs=pl.BlockSpec(memory_space=pltpu.VMEM),
        scratch_shapes=[pltpu.VMEM(values.shape, jnp.float32), pltpu.SemaphoreType.DMA, pltpu.SemaphoreType.DMA],
        compiler_params=pltpu.CompilerParams(collective_id=ident, has_side_effects=True),
    )(values)


def total(values, ident):
    devices = values.shape[0]
    return pl.pallas_call(
        functools.partial(total_kernel, devices),
        out_shape=jax.ShapeDtypeStruct(values.shape, jnp.float32),
        in_specs=[pl.BlockSpec(memory_space=pltpu.VMEM)],
        out_specs=pl.BlockSpec(memory_space=pltpu.VMEM),
        scratch_shapes=[
            pltpu.VMEM(values.shape, jnp.float32),
            pltpu.VMEM(values.shape[1:], jnp.float32),
            pltpu.VMEM(values.shape, jnp.float32),
            pltpu.SemaphoreType.DMA((4,)),
        ],
        compiler_params=pltpu.CompilerParams(collective_id=ident, has_side_effects=True),
    )(values)


def shards(tensor, factor_two, factor_three, factor_four, factor_init):
    axes = ("row", "col")
    first_len, local_two, width = tensor.shape
    fourth_len, rank_four = factor_four.shape
    local_three = width // fourth_len
    rank_one = factor_init.shape[1]
    rows, cols = lax.axis_size("row"), lax.axis_size("col")
    devices = rows * cols
    local_pairs = local_two * local_three
    features = rank_four * rank_one
    part = features // devices
    data = tensor.reshape(first_len, local_pairs, fourth_len)
    rank_two, rank_three = factor_two.shape[1], factor_three.shape[1]

    def pull(vectors):
        mixed = jnp.einsum("apd,ar->prd", data, vectors, precision=HIGHEST)
        return jnp.einsum("prd,de->per", mixed, factor_four, precision=HIGHEST).reshape(local_pairs, features)

    def share(values, ident):
        length = values.shape[1]
        padded = -(-length // LANES) * LANES
        values = jnp.pad(values, ((0, 0), (0, padded - length))).reshape(devices, padded // LANES, LANES)
        return swap(values, ident).reshape(devices, padded)[:, :length]

    def spread(block, ident, extra=None):
        put = block.reshape(local_pairs, devices, part).transpose(1, 0, 2).reshape(devices, local_pairs * part)
        if extra is not None:
            put = jnp.concatenate([put, jnp.broadcast_to(extra[None], (devices, extra.shape[0]))], axis=1)
        got = share(put, ident)
        rest = got[:, local_pairs * part:]
        got = got[:, :local_pairs * part]
        got = got.reshape(rows, cols, local_two, local_three, part)
        return got.transpose(0, 2, 1, 3, 4).reshape(rows * local_two, cols * local_three, part), rest

    def gather(block, ident):
        two, three, _ = block.shape
        put = block.reshape(rows, two // rows, cols, three // cols, part).transpose(0, 2, 1, 3, 4)
        got = share(put.reshape(devices, -1), ident).reshape(devices, (two // rows) * (three // cols), part)
        return got.transpose(1, 0, 2).reshape(got.shape[1], features)

    extra = jnp.concatenate([factor_two.reshape(-1), factor_three.reshape(-1)])
    block, rest = spread(pull(factor_init), 1, extra)
    rest = rest.reshape(rows, cols, -1)
    whole_two = rest[:, 0, :factor_two.size].reshape(-1, rank_two)
    whole_three = rest[0, :, factor_two.size:].reshape(-1, rank_three)
    block = jnp.einsum("bcq,bg->gcq", block, whole_two, precision=HIGHEST)
    block = jnp.einsum("gcq,cf->gfq", block, whole_three, precision=HIGHEST)
    block = jnp.einsum("gfq,cf->gcq", block, whole_three, precision=HIGHEST)
    block = jnp.einsum("gcq,bg->bcq", block, whole_two, precision=HIGHEST)
    block = gather(block, 2).reshape(local_pairs, rank_four, rank_one)
    block = jnp.einsum("per,de->pdr", block, factor_four, precision=HIGHEST)
    image = dot(tensor.reshape(first_len, -1), block.reshape(-1, rank_one), ((1,), (0,)))
    half = first_len // 2
    image = jnp.concatenate([image[:half], image[half:]], axis=1).reshape(devices, half // devices, 2 * rank_one)
    image = total(image, 0).reshape(half, 2 * rank_one)
    image = jnp.concatenate([image[:, :rank_one], image[:, rank_one:]], axis=0)
    basis, inverse = finish(image)
    block, _ = spread(pull(image), 3)
    block = jnp.einsum("bcq,bg->gcq", block, whole_two, precision=HIGHEST)
    block = jnp.einsum("gcq,cf->gfq", block, whole_three, precision=HIGHEST)
    block = gather(block, 4).reshape(-1, rank_four, rank_one)
    core = jnp.einsum("per,sr->spe", block, inverse, precision=HIGHEST)
    return (basis, core.reshape(rank_one, rank_two // rows, rank_three // cols, rank_four))


def solution(mesh):
    in_specs = (P(None, "row", "col"), P("row", None), P("col", None), P(), P())
    out_specs = (P(), P(None, "row", "col", None))
    return jax.shard_map(shards, mesh=mesh, in_specs=in_specs, out_specs=out_specs, check_vma=False)
```

```python
import functools

import jax
import jax.numpy as jnp
from jax import lax
from jax.experimental import pallas as pl
from jax.experimental.pallas import tpu as pltpu
from jax.sharding import PartitionSpec as P

HIGHEST = lax.Precision.HIGHEST
LANES = 128


def dot(a, b, dims):
    return lax.dot_general(a, b, (dims, ((), ())), precision=HIGHEST, preferred_element_type=jnp.float32)


def inverse_factor(square):
    size = square.shape[0]
    rows = lax.broadcasted_iota(jnp.int32, (size, size), 0)
    cols = lax.broadcasted_iota(jnp.int32, (size, size), 1)
    index = lax.broadcasted_iota(jnp.int32, (size, 1), 0)
    left = square
    right = jnp.where(rows == cols, 1.0, 0.0).astype(jnp.float32)
    for k in range(size):
        scale = lax.rsqrt(left[k:k + 1, k:k + 1])
        column = left[:, k:k + 1] * scale
        pivot_left = left[k:k + 1, :] * scale
        pivot_right = right[k:k + 1, :] * scale
        factor = jnp.where(index > k, column, 0.0)
        left = left - factor * pivot_left
        right = jnp.where(index == k, pivot_right, right - factor * pivot_right)
    return right


def finish_kernel(image_ref, basis_ref, inverse_ref):
    image = image_ref[...]
    inverse = inverse_factor(dot(image, image, ((0,), (0,))))
    inverse_ref[...] = inverse
    basis_ref[...] = dot(image, inverse, ((1,), (1,)))


def finish(image):
    rank = image.shape[1]
    return pl.pallas_call(
        finish_kernel,
        out_shape=(
            jax.ShapeDtypeStruct(image.shape, jnp.float32),
            jax.ShapeDtypeStruct((rank, rank), jnp.float32),
        ),
    )(image)


def place():
    return lax.axis_index("row") * lax.axis_size("col") + lax.axis_index("col")


def greet(devices):
    cols = lax.axis_size("col")
    me = place()
    barrier = pltpu.get_barrier_semaphore()

    def hello(k, carry):
        peer = lax.rem(me + k, devices)
        pl.semaphore_signal(barrier, inc=1, device_id=(peer // cols, lax.rem(peer, cols)), device_id_type=pl.DeviceIdType.MESH)
        return carry

    lax.fori_loop(1, devices, hello, 0)
    pl.semaphore_wait(barrier, devices - 1)


def send_all(devices, source, target, send_sem, recv_sem):
    cols = lax.axis_size("col")
    me = place()

    def send(k, carry):
        peer = lax.rem(me + k, devices)
        pltpu.make_async_remote_copy(
            src_ref=source(peer),
            dst_ref=target.at[me],
            send_sem=send_sem,
            recv_sem=recv_sem,
            device_id=(peer // cols, lax.rem(peer, cols)),
            device_id_type=pl.DeviceIdType.MESH,
        ).start()
        return carry

    lax.fori_loop(1, devices, send, 0)
    whole = target.at[pl.ds(0, devices - 1)]
    pltpu.make_async_copy(whole, whole, send_sem).wait()
    pltpu.make_async_copy(whole, whole, recv_sem).wait()


def swap_kernel(devices, put_ref, out_ref, held, send_sem, recv_sem):
    me = place()
    greet(devices)
    send_all(devices, lambda peer: put_ref.at[peer], held, send_sem, recv_sem)
    held[me] = put_ref[me]
    out_ref[...] = held[...]


def total_kernel(devices, put_ref, out_ref, held, mine, spread, sems):
    me = place()
    greet(devices)
    send_all(devices, lambda peer: put_ref.at[peer], held, sems.at[0], sems.at[1])
    held[me] = put_ref[me]
    mine[...] = jnp.sum(held[...], axis=0)
    send_all(devices, lambda peer: mine, spread, sems.at[2], sems.at[3])
    spread[me] = mine[...]
    out_ref[...] = spread[...]


def swap(values, ident):
    devices = values.shape[0]
    return pl.pallas_call(
        functools.partial(swap_kernel, devices),
        out_shape=jax.ShapeDtypeStruct(values.shape, jnp.float32),
        in_specs=[pl.BlockSpec(memory_space=pltpu.VMEM)],
        out_specs=pl.BlockSpec(memory_space=pltpu.VMEM),
        scratch_shapes=[pltpu.VMEM(values.shape, jnp.float32), pltpu.SemaphoreType.DMA, pltpu.SemaphoreType.DMA],
        compiler_params=pltpu.CompilerParams(collective_id=ident, has_side_effects=True),
    )(values)


def total(values, ident):
    devices = values.shape[0]
    return pl.pallas_call(
        functools.partial(total_kernel, devices),
        out_shape=jax.ShapeDtypeStruct(values.shape, jnp.float32),
        in_specs=[pl.BlockSpec(memory_space=pltpu.VMEM)],
        out_specs=pl.BlockSpec(memory_space=pltpu.VMEM),
        scratch_shapes=[
            pltpu.VMEM(values.shape, jnp.float32),
            pltpu.VMEM(values.shape[1:], jnp.float32),
            pltpu.VMEM(values.shape, jnp.float32),
            pltpu.SemaphoreType.DMA((4,)),
        ],
        compiler_params=pltpu.CompilerParams(collective_id=ident, has_side_effects=True),
    )(values)


def shards(tensor, factor_two, factor_three, factor_four, factor_init):
    axes = ("row", "col")
    first_len, local_two, width = tensor.shape
    fourth_len, rank_four = factor_four.shape
    local_three = width // fourth_len
    rank_one = factor_init.shape[1]
    rows, cols = lax.axis_size("row"), lax.axis_size("col")
    devices = rows * cols
    local_pairs = local_two * local_three
    features = rank_four * rank_one
    part = features // devices
    data = tensor.reshape(first_len, local_pairs, fourth_len)
    rank_two, rank_three = factor_two.shape[1], factor_three.shape[1]

    def pull(vectors):
        mixed = jnp.einsum("apd,ar->prd", data, vectors, precision=lax.Precision.HIGH)
        return jnp.einsum("prd,de->per", mixed, factor_four, precision=HIGHEST).reshape(local_pairs, features)

    def share(values, ident):
        length = values.shape[1]
        padded = -(-length // LANES) * LANES
        values = jnp.pad(values, ((0, 0), (0, padded - length))).reshape(devices, padded // LANES, LANES)
        return swap(values, ident).reshape(devices, padded)[:, :length]

    def spread(block, ident, extra=None):
        put = block.reshape(local_pairs, devices, part).transpose(1, 0, 2).reshape(devices, local_pairs * part)
        if extra is not None:
            put = jnp.concatenate([put, jnp.broadcast_to(extra[None], (devices, extra.shape[0]))], axis=1)
        got = share(put, ident)
        rest = got[:, local_pairs * part:]
        got = got[:, :local_pairs * part]
        got = got.reshape(rows, cols, local_two, local_three, part)
        return got.transpose(0, 2, 1, 3, 4).reshape(rows * local_two, cols * local_three, part), rest

    def gather(block, ident):
        two, three, _ = block.shape
        put = block.reshape(rows, two // rows, cols, three // cols, part).transpose(0, 2, 1, 3, 4)
        got = share(put.reshape(devices, -1), ident).reshape(devices, (two // rows) * (three // cols), part)
        return got.transpose(1, 0, 2).reshape(got.shape[1], features)

    extra = jnp.concatenate([factor_two.reshape(-1), factor_three.reshape(-1)])
    block, rest = spread(pull(factor_init), 1, extra)
    rest = rest.reshape(rows, cols, -1)
    whole_two = rest[:, 0, :factor_two.size].reshape(-1, rank_two)
    whole_three = rest[0, :, factor_two.size:].reshape(-1, rank_three)
    block = jnp.einsum("bcq,bg->gcq", block, whole_two, precision=HIGHEST)
    block = jnp.einsum("gcq,cf->gfq", block, whole_three, precision=HIGHEST)
    block = jnp.einsum("gfq,cf->gcq", block, whole_three, precision=HIGHEST)
    block = jnp.einsum("gcq,bg->bcq", block, whole_two, precision=HIGHEST)
    block = gather(block, 2).reshape(local_pairs, rank_four, rank_one)
    block = jnp.einsum("per,de->pdr", block, factor_four, precision=HIGHEST)
    image = jnp.dot(tensor.reshape(first_len, -1), block.reshape(-1, rank_one), precision=lax.Precision.HIGH)
    half = first_len // 2
    image = jnp.concatenate([image[:half], image[half:]], axis=1).reshape(devices, half // devices, 2 * rank_one)
    image = total(image, 0).reshape(half, 2 * rank_one)
    image = jnp.concatenate([image[:, :rank_one], image[:, rank_one:]], axis=0)
    basis, inverse = finish(image)
    block, _ = spread(pull(image), 3)
    block = jnp.einsum("bcq,bg->gcq", block, whole_two, precision=HIGHEST)
    block = jnp.einsum("gcq,cf->gfq", block, whole_three, precision=HIGHEST)
    block = gather(block, 4).reshape(-1, rank_four, rank_one)
    core = jnp.einsum("per,sr->spe", block, inverse, precision=HIGHEST)
    return (basis, core.reshape(rank_one, rank_two // rows, rank_three // cols, rank_four))


def solution(mesh):
    in_specs = (P(None, "row", "col"), P("row", None), P("col", None), P(), P())
    out_specs = (P(), P(None, "row", "col", None))
    return jax.shard_map(shards, mesh=mesh, in_specs=in_specs, out_specs=out_specs, check_vma=False)
```
